8 devices in a mesh: dp: 1 (over z), cy: 2 (over y), cx: 4 (over x, core).
Axes of the slice: x: 2, y: 2, z: 1, core: 2. Of those that a mesh axis runs over, the one named last changes fastest.
Arguments:
- query_rows: bfloat16 [8192, 28, 128], P(('dp', 'cy', 'cx'))
- key_rows: bfloat16 [8192, 4, 128], P(('dp', 'cy', 'cx'))
- value_rows: bfloat16 [8192, 4, 128], P(('dp', 'cy', 'cx'))
- out_rows: bfloat16 [8192, 28, 128], P(('dp', 'cy', 'cx'))
- grad_out: bfloat16 [8192, 28, 128], P(('dp', 'cy', 'cx'))
- log_sum_exp: float32 [8192, 28], P(('dp', 'cy', 'cx'))
Outputs:
- output 1: bfloat16 [8192, 28, 128], P(('dp', 'cy', 'cx'))
- output 2: bfloat16 [8192, 4, 128], P(('dp', 'cy', 'cx'))
- output 3: bfloat16 [8192, 4, 128], P(('dp', 'cy', 'cx'))
All inputs are finite; a program needn't handle non-finite values.
Results may differ from the reference program's by a relative error of at most 0.00401.
Values are sent between devices in bfloat16 or wider.
A program may use at most 1 GiB of HBM per device.

```python
import math
import jax
import jax.numpy as jnp
from jax import lax

Q_HEADS = 28
KV_HEADS = 4
HEAD_DIM = 128
TOK_DEV = 1024
CTX_DEVS = 8
ROW_BLOCK = 64
SEQ_LEN = CTX_DEVS * TOK_DEV
CHUNK_LEN = TOK_DEV // 2
GROUP_SIZE = Q_HEADS // KV_HEADS
N_BLOCKS = SEQ_LEN // ROW_BLOCK
SCALING = 1.0 / math.sqrt(HEAD_DIM)


def seq_positions():
    local_idx = jnp.arange(TOK_DEV, dtype=jnp.int32)
    dev_idx = jnp.arange(CTX_DEVS, dtype=jnp.int32)
    piece_id = jnp.where(local_idx[None, :] < CHUNK_LEN, dev_idx[:, None], 2 * CTX_DEVS - 1 - dev_idx[:, None])
    return (piece_id * CHUNK_LEN + local_idx[None, :] % CHUNK_LEN).reshape(SEQ_LEN)


def to_seq_order(row_data):
    split_rows = row_data.reshape((CTX_DEVS, 2, CHUNK_LEN) + row_data.shape[1:])
    return jnp.concatenate([split_rows[:, 0], split_rows[::-1, 1]], axis=0).reshape(row_data.shape)


def to_device_order(row_data):
    split_rows = row_data.reshape((2, CTX_DEVS, CHUNK_LEN) + row_data.shape[1:])
    return jnp.stack([split_rows[0], split_rows[1, ::-1]], axis=1).reshape(row_data.shape)


def forward_stats(q_seq, k_seq, v_seq):
    keys_f32 = k_seq.astype(jnp.float32)
    vals_f32 = v_seq.astype(jnp.float32)
    key_pos = jnp.arange(SEQ_LEN)
    q_blocks = q_seq.reshape(N_BLOCKS, ROW_BLOCK, KV_HEADS, GROUP_SIZE, HEAD_DIM)

    def one_block(block_in):
        q_blk, blk_idx = block_in
        query_pos = blk_idx * ROW_BLOCK + jnp.arange(ROW_BLOCK)
        keep_mask = (query_pos[:, None] >= key_pos[None, :])[None, None]
        scores = jnp.einsum('bkgd,skd->kgbs', q_blk.astype(jnp.float32), keys_f32) * SCALING
        masked = jnp.where(keep_mask, scores, -1e30)
        row_max = jnp.max(masked, axis=-1)
        exp_vals = jnp.exp(masked - row_max[..., None])
        row_sum = jnp.sum(exp_vals, axis=-1)
        prob_b16 = (exp_vals / row_sum[..., None]).astype(jnp.bfloat16)
        out_blk = jnp.einsum('kgbs,skd->bkgd', prob_b16.astype(jnp.float32), vals_f32)
        lse_blk = (row_max + jnp.log(row_sum)).transpose(2, 0, 1)
        return out_blk.astype(jnp.bfloat16).reshape(ROW_BLOCK, Q_HEADS, HEAD_DIM), lse_blk.reshape(ROW_BLOCK, Q_HEADS)

    out_blocks, lse_blocks = lax.map(one_block, (q_blocks, jnp.arange(N_BLOCKS)))
    return out_blocks.reshape(SEQ_LEN, Q_HEADS, HEAD_DIM), lse_blocks.reshape(SEQ_LEN, Q_HEADS)


def setup_inputs(seed: int = 0, part: int = 0) -> dict:
    root_key = jax.random.fold_in(jax.random.key(seed), part)
    sub_keys = jax.random.split(root_key, 6)
    shape_q = (SEQ_LEN, Q_HEADS, HEAD_DIM)
    shape_kv = (SEQ_LEN, KV_HEADS, HEAD_DIM)
    query_f32 = jax.random.normal(sub_keys[0], shape_q, jnp.float32)
    key_mean = jax.random.normal(sub_keys[1], (KV_HEADS, HEAD_DIM), jnp.float32)
    key_f32 = jax.random.normal(sub_keys[2], shape_kv, jnp.float32) + key_mean
    value_mean = jax.random.normal(sub_keys[3], (KV_HEADS, HEAD_DIM), jnp.float32)
    value_f32 = jax.random.normal(sub_keys[4], shape_kv, jnp.float32) + value_mean
    row_pos = seq_positions().astype(jnp.float32)
    dout_f32 = jax.random.normal(sub_keys[5], shape_q, jnp.float32) * jnp.sqrt((row_pos + 1.0) / 4.0)[:, None, None]
    query_rows = query_f32.astype(jnp.bfloat16)
    key_rows = key_f32.astype(jnp.bfloat16)
    value_rows = value_f32.astype(jnp.bfloat16)
    out_seq, lse_seq = forward_stats(to_seq_order(query_rows), to_seq_order(key_rows), to_seq_order(value_rows))
    return {'query_rows': query_rows, 'key_rows': key_rows, 'value_rows': value_rows, 'out_rows': to_device_order(out_seq), 'grad_out': dout_f32.astype(jnp.bfloat16), 'log_sum_exp': to_device_order(lse_seq)}


def reference(query_rows, key_rows, value_rows, out_rows, grad_out, log_sum_exp):
    q_seq = to_seq_order(query_rows)
    keys_f32 = to_seq_order(key_rows).astype(jnp.float32)
    vals_f32 = to_seq_order(value_rows).astype(jnp.float32)
    do_seq = to_seq_order(grad_out)
    delta_seq = jnp.einsum('shd,shd->sh', do_seq.astype(jnp.float32), to_seq_order(out_rows).astype(jnp.float32))
    lse_seq = to_seq_order(log_sum_exp)
    blk_shape = (N_BLOCKS, ROW_BLOCK, KV_HEADS, GROUP_SIZE)
    key_pos = jnp.arange(SEQ_LEN)

    def one_block(grad_acc, block_in):
        dk_acc, dv_acc = grad_acc
        q_blk, do_blk, lse_blk, delta_blk, blk_idx = block_in
        q_f32 = q_blk.astype(jnp.float32)
        do_f32 = do_blk.astype(jnp.float32)
        query_pos = blk_idx * ROW_BLOCK + jnp.arange(ROW_BLOCK)
        keep_mask = (query_pos[:, None] >= key_pos[None, :])[None, None]
        scores = jnp.einsum('bkgd,skd->kgbs', q_f32, keys_f32) * SCALING
        prob_f32 = jnp.where(keep_mask, jnp.exp(scores - lse_blk.transpose(1, 2, 0)[..., None]), 0.0)
        dprob_f32 = jnp.einsum('bkgd,skd->kgbs', do_f32, vals_f32)
        dscore = (prob_f32 * (dprob_f32 - delta_blk.transpose(1, 2, 0)[..., None])).astype(jnp.bfloat16).astype(jnp.float32)
        prob_rnd = prob_f32.astype(jnp.bfloat16).astype(jnp.float32)
        dq_blk = jnp.einsum('kgbs,skd->bkgd', dscore, keys_f32) * SCALING
        dk_acc = dk_acc + jnp.einsum('kgbs,bkgd->skd', dscore, q_f32)
        dv_acc = dv_acc + jnp.einsum('kgbs,bkgd->skd', prob_rnd, do_f32)
        return (dk_acc, dv_acc), dq_blk.astype(jnp.bfloat16).reshape(ROW_BLOCK, Q_HEADS, HEAD_DIM)

    zero_kv = jnp.zeros((SEQ_LEN, KV_HEADS, HEAD_DIM), jnp.float32)
    block_ins = (q_seq.reshape(blk_shape + (HEAD_DIM,)), do_seq.reshape(blk_shape + (HEAD_DIM,)), lse_seq.reshape(blk_shape), delta_seq.reshape(blk_shape), jnp.arange(N_BLOCKS))
    (dk_acc, dv_acc), dq_blocks = lax.scan(one_block, (zero_kv, zero_kv), block_ins)
    grad_query = to_device_order(dq_blocks.reshape(SEQ_LEN, Q_HEADS, HEAD_DIM))
    grad_key = to_device_order((dk_acc * SCALING).astype(jnp.bfloat16))
    grad_value = to_device_order(dv_acc.astype(jnp.bfloat16))
    return grad_query, grad_key, grad_value
```

```python
import math
import jax
import jax.numpy as jnp
from jax import lax
from jax.experimental import pallas as pl
from jax.experimental.pallas import tpu as pltpu
from jax.sharding import PartitionSpec as P

LOG2E = math.log2(math.e)
F32 = jnp.float32
BF16 = jnp.bfloat16
Q_TILE = 256


def group_kernel(n_piece, tab_ref, q_ref, do_ref, lse_ref, delta_ref, k_ref, v_ref, dq_ref, dkv_ref, kt_scr, vt_scr, p_scr, ds_scr, dk_acc, dv_acc, dq_acc):
    n_head, tok_dev, head_dim = q_ref.shape
    half_tok = tok_dev // 2
    scaling = 1.0 / math.sqrt(head_dim)
    step = pl.program_id(0)
    q_half = tab_ref[step, 1]
    kind = tab_ref[step, 2]
    is_first = tab_ref[step, 3]
    is_last = tab_ref[step, 4]
    n_sub = half_tok // Q_TILE

    @pl.when(step == 0)
    def _():
        dq_acc[...] = jnp.zeros_like(dq_acc)

    @pl.when(is_first == 1)
    def _():
        dk_acc[...] = jnp.zeros_like(dk_acc)
        dv_acc[...] = jnp.zeros_like(dv_acc)

    def run_task(masked):
        kt_scr[...] = k_ref[...].T
        vt_scr[...] = v_ref[...].T
        row0 = pl.multiple_of(q_half * half_tok, half_tok)

        def scores(h, sub, slot):
            rows = pl.ds(row0 + sub * Q_TILE, Q_TILE)
            n_key = half_tok if not masked else (sub + 1) * Q_TILE
            s = jnp.dot(q_ref[h, rows, :], kt_scr[:, :n_key], preferred_element_type=F32)
            dp = jnp.dot(do_ref[h, rows, :], vt_scr[:, :n_key], preferred_element_type=F32)
            lse = jnp.tile(lse_ref[h, rows, :], (1, n_key // 128))
            dlt = jnp.tile(delta_ref[h, rows, :], (1, n_key // 128))
            prob = jnp.exp2(s * (scaling * LOG2E) - lse)
            if masked:
                qi = lax.broadcasted_iota(jnp.int32, s.shape, 0) + sub * Q_TILE
                kj = lax.broadcasted_iota(jnp.int32, s.shape, 1)
                prob = jnp.where(qi >= kj, prob, 0.0)
            p_scr[slot, :, :n_key] = prob.astype(BF16)
            ds_scr[slot, :, :n_key] = (prob * (dp - dlt)).astype(BF16)

        def grads(h, sub, slot):
            rows = pl.ds(row0 + sub * Q_TILE, Q_TILE)
            n_key = half_tok if not masked else (sub + 1) * Q_TILE
            prob = p_scr[slot, :, :n_key]
            ds = ds_scr[slot, :, :n_key]
            dv_acc[:, :n_key] += lax.dot_general(do_ref[h, rows, :], prob, (((0,), (0,)), ((), ())), preferred_element_type=F32)
            dk_acc[:, :n_key] += lax.dot_general(q_ref[h, rows, :], ds, (((0,), (0,)), ((), ())), preferred_element_type=F32)
            dq_acc[h, rows, :] += jnp.dot(ds, k_ref[:n_key, :], preferred_element_type=F32)

        tiles = [(h, sub) for h in range(n_head) for sub in range(n_sub)]
        scores(*tiles[0], 0)
        for idx, tile in enumerate(tiles):
            if idx + 1 < len(tiles):
                scores(*tiles[idx + 1], (idx + 1) % 2)
            grads(*tile, idx % 2)

    @pl.when(kind == 1)
    def _():
        run_task(False)

    @pl.when(kind == 2)
    def _():
        run_task(True)

    @pl.when(is_last == 1)
    def _():
        dkv_ref[0] = dk_acc[...].T * scaling
        dkv_ref[1] = dv_acc[...].T

    @pl.when(step == pl.num_programs(0) - 1)
    def _():
        dq_ref[...] = (dq_acc[...] * scaling).astype(BF16)


def solution(mesh):
    n_cx = mesh.shape['cx']
    n_ctx = mesh.shape['cy'] * n_cx
    ctx_axes = ('cy', 'cx')
    row_spec = P(('dp', 'cy', 'cx'), None, None)
    stat_spec = P(('dp', 'cy', 'cx'), None)

    def local_grads(query_rows, key_rows, value_rows, out_rows, grad_out, log_sum_exp):
        tok_dev, n_heads, head_dim = query_rows.shape
        kv_heads = key_rows.shape[1]
        group_size = n_heads // kv_heads
        half_tok = tok_dev // 2
        n_piece = 2 * n_ctx
        n_step = 2 * n_piece - n_ctx
        ctx_rank = lax.axis_index('cy') * n_cx + lax.axis_index('cx')

        step = jnp.arange(n_step, dtype=jnp.int32)
        both = step < 2 * ctx_rank + 2
        piece = jnp.where(both, step // 2, step - ctx_rank - 1)
        idle = piece > n_piece - 1
        piece = jnp.minimum(piece, n_piece - 1)
        q_half = jnp.where(both, step % 2, 1)
        late = n_piece - 1 - ctx_rank
        diag = jnp.where(q_half == 0, piece == ctx_rank, piece == late)
        kind = jnp.where(idle | (piece > late), 0, jnp.where(diag, 2, 1))
        first = jnp.where(idle, 0, jnp.where(both, 1 - q_half, 1))
        last = jnp.where(idle, 0, q_half)
        slot = jnp.where(piece < n_ctx, 2 * piece, 2 * (n_piece - 1 - piece) + 1)
        table = jnp.stack([slot, q_half, kind, first, last], axis=1).astype(jnp.int32)

        def heads_first(rows):
            return rows.reshape(tok_dev, kv_heads, group_size, head_dim).transpose(1, 2, 0, 3)

        def lanes(stat):
            stat_t = stat.reshape(tok_dev, kv_heads, group_size).transpose(1, 2, 0)
            return jnp.broadcast_to(stat_t[..., None], stat_t.shape + (128,))

        kv_rows = jnp.stack([key_rows, value_rows]).transpose(2, 0, 1, 3)
        kv_all = [lax.all_gather(kv_rows[g], ctx_axes) for g in range(kv_heads)]
        delta = jnp.einsum('thd,thd->th', grad_out, out_rows, preferred_element_type=F32)
        q_hf, do_hf = heads_first(query_rows), heads_first(grad_out)
        lse_l, delta_l = lanes(log_sum_exp * LOG2E), lanes(delta)

        call = pl.pallas_call(
            lambda *refs: group_kernel(n_piece, *refs),
            grid_spec=pltpu.PrefetchScalarGridSpec(
                num_scalar_prefetch=1,
                grid=(n_step,),
                in_specs=[
                    pl.BlockSpec((group_size, tok_dev, head_dim), lambda t, tab: (0, 0, 0), pipeline_mode=pl.Buffered(1)),
                    pl.BlockSpec((group_size, tok_dev, head_dim), lambda t, tab: (0, 0, 0), pipeline_mode=pl.Buffered(1)),
                    pl.BlockSpec((group_size, tok_dev, 128), lambda t, tab: (0, 0, 0), pipeline_mode=pl.Buffered(1)),
                    pl.BlockSpec((group_size, tok_dev, 128), lambda t, tab: (0, 0, 0), pipeline_mode=pl.Buffered(1)),
                    pl.BlockSpec((None, None, None, half_tok, head_dim), lambda t, tab: (tab[t, 0] // 2, 0, tab[t, 0] % 2, 0, 0)),
                    pl.BlockSpec((None, None, None, half_tok, head_dim), lambda t, tab: (tab[t, 0] // 2, 1, tab[t, 0] % 2, 0, 0)),
                ],
                out_specs=[
                    pl.BlockSpec((group_size, tok_dev, head_dim), lambda t, tab: (0, 0, 0), pipeline_mode=pl.Buffered(1)),
                    pl.BlockSpec((None, 2, None, half_tok, head_dim), lambda t, tab: (tab[t, 0] // 2, 0, tab[t, 0] % 2, 0, 0)),
                ],
                scratch_shapes=[
                    pltpu.VMEM((head_dim, half_tok), BF16),
                    pltpu.VMEM((head_dim, half_tok), BF16),
                    pltpu.VMEM((2, Q_TILE, half_tok), BF16),
                    pltpu.VMEM((2, Q_TILE, half_tok), BF16),
                    pltpu.VMEM((head_dim, half_tok), F32),
                    pltpu.VMEM((head_dim, half_tok), F32),
                    pltpu.VMEM((group_size, tok_dev, head_dim), F32),
                ],
            ),
            out_shape=[
                jax.ShapeDtypeStruct((group_size, tok_dev, head_dim), BF16),
                jax.ShapeDtypeStruct((n_ctx, 2, 2, half_tok, head_dim), F32),
            ],
            compiler_params=pltpu.CompilerParams(dimension_semantics=('arbitrary',), vmem_limit_bytes=48 * 1024 * 1024),
            cost_estimate=pl.CostEstimate(flops=17 * group_size * 10 * half_tok * half_tok * head_dim, bytes_accessed=32 * 1024 * 1024, transcendentals=17 * group_size * half_tok * half_tok),
            name='group_grads',
        )

        dq_parts, dkv_parts = [], []
        for g in range(kv_heads):
            kv_g = kv_all[g].reshape(n_ctx, 2, 2, half_tok, head_dim)
            dq_g, dkv_g = call(table, q_hf[g], do_hf[g], lse_l[g], delta_l[g], kv_g, kv_g)
            dq_parts.append(dq_g)
            dkv_parts.append(lax.psum_scatter(dkv_g, ctx_axes, scatter_dimension=0, tiled=False))
        grad_query = jnp.stack(dq_parts).transpose(2, 0, 1, 3).reshape(tok_dev, n_heads, head_dim)
        dkv = jnp.stack([x.reshape(2, tok_dev, head_dim) for x in dkv_parts], axis=2)
        dkv_b16 = dkv.astype(BF16)
        return grad_query, dkv_b16[0], dkv_b16[1]

    return jax.shard_map(local_grads, mesh=mesh, in_specs=(row_spec, row_spec, row_spec, row_spec, row_spec, stat_spec), out_specs=(row_spec, row_spec, row_spec), check_vma=False)
```

```python
import functools
import math
import numpy as np
import jax
import jax.numpy as jnp
from jax import lax
from jax.experimental import pallas as pl
from jax.experimental.pallas import tpu as pltpu
from jax.sharding import PartitionSpec as P

LOG2E = math.log2(math.e)
F32 = jnp.float32
BF16 = jnp.bfloat16
Q_TILE = 256
N_PART = 3


def task_table(n_ctx, peers):
    tables = []
    for rank in range(n_ctx):
        chip, core = rank // 2, rank % 2

        def ids(chip_id):
            devs = (2 * chip_id + core, 2 * chip_id + 1 - core)
            return [dev if half == 0 else 2 * n_ctx - 1 - dev for dev in devs for half in range(2)]

        rows = []
        keys = [piece for peer in peers for piece in ids(chip ^ peer)]
        for q_slot, q_id in enumerate(ids(chip)):
            todo = [(k_slot, 2 if k_id == q_id else 1) for k_slot, k_id in enumerate(keys) if k_id <= q_id]
            todo = todo or [(rows[-1][1] if rows else 0, 0)]
            for n, (k_slot, kind) in enumerate(todo):
                rows.append([q_slot, k_slot, kind, int(n == 0), int(n == len(todo) - 1)])
        tables.append(rows)
    n_step = max(len(rows) for rows in tables)
    for rows in tables:
        while len(rows) < n_step:
            rows.append([rows[-1][0], rows[-1][1], 3, 0, 0])
    return np.array(tables, np.int32)


def block_kernel(has_in, is_end, has_diag, tab_ref, q_ref, do_ref, aug_ref, k_ref, v_ref, *refs):
    if has_in:
        dqi_ref, *refs = refs
    dq_ref, dkv_ref, kt_scr, vt_scr, p_scr, ds_scr, *refs = refs
    dq_acc = refs[0] if is_end else dq_ref
    n_head, n_row, head_dim = q_ref.shape
    scaling = 1.0 / math.sqrt(head_dim)
    step = pl.program_id(0)
    k_slot = tab_ref[step, 1]
    kind = tab_ref[step, 2]
    is_first = tab_ref[step, 3]
    is_last = tab_ref[step, 4]
    n_sub = n_row // Q_TILE

    @pl.when(step == 0)
    def _():
        dkv_ref[...] = jnp.zeros_like(dkv_ref)
        row_id = lax.broadcasted_iota(jnp.int32, (head_dim, n_row), 0)
        kt_scr[head_dim:, :] = jnp.where(row_id < N_PART, -1.0, 0.0).astype(BF16)
        vt_scr[head_dim:, :] = jnp.where((row_id >= N_PART) & (row_id < 2 * N_PART), -1.0, 0.0).astype(BF16)

    def run_task(masked):
        kt_scr[:head_dim, :] = k_ref[...].T
        vt_scr[:head_dim, :] = v_ref[...].T
        fresh = is_first == 1

        def scores(h, sub, slot):
            rows = pl.ds(sub * Q_TILE, Q_TILE)
            n_key = n_row if not masked else (sub + 1) * Q_TILE
            aug = aug_ref[h, rows, :]
            s = jnp.dot(jnp.concatenate([q_ref[h, rows, :], aug], axis=1), kt_scr[:, :n_key], preferred_element_type=F32)
            dp = jnp.dot(jnp.concatenate([do_ref[h, rows, :], aug], axis=1), vt_scr[:, :n_key], preferred_element_type=F32)
            prob = jnp.exp2(s * (scaling * LOG2E))
            if masked:
                qi = lax.broadcasted_iota(jnp.int32, s.shape, 0) + sub * Q_TILE
                kj = lax.broadcasted_iota(jnp.int32, s.shape, 1)
                prob = jnp.where(qi >= kj, prob, 0.0)
            p_scr[slot, :, :n_key] = prob.astype(BF16)
            ds_scr[slot, :, :n_key] = (prob * dp).astype(BF16)

        def grads(h, sub, slot):
            rows = pl.ds(sub * Q_TILE, Q_TILE)
            n_key = n_row if not masked else (sub + 1) * Q_TILE
            prob = p_scr[slot, :, :n_key]
            ds = ds_scr[slot, :, :n_key]
            dkv_ref[1, k_slot, :, :n_key] += lax.dot_general(do_ref[h, rows, :], prob, (((0,), (0,)), ((), ())), preferred_element_type=F32)
            dkv_ref[0, k_slot, :, :n_key] += lax.dot_general(q_ref[h, rows, :], ds, (((0,), (0,)), ((), ())), preferred_element_type=F32)
            base = jnp.where(fresh, dqi_ref[h, :, rows] if has_in else 0.0, dq_acc[h, :, rows])
            dq_acc[h, :, rows] = base + lax.dot_general(kt_scr[:head_dim, :n_key], ds, (((1,), (1,)), ((), ())), preferred_element_type=F32)

        tiles = [(h, sub) for h in range(n_head) for sub in range(n_sub)]
        scores(*tiles[0], 0)
        for idx, tile in enumerate(tiles):
            if idx + 1 < len(tiles):
                scores(*tiles[idx + 1], (idx + 1) % 2)
            grads(*tile, idx % 2)

    @pl.when(kind == 1)
    def _():
        run_task(False)

    if has_diag:
        @pl.when(kind == 2)
        def _():
            run_task(True)
    else:
        @pl.when(kind == 0)
        def _():
            dq_acc[...] = dqi_ref[...] if has_in else jnp.zeros_like(dq_acc)

    if is_end:
        @pl.when(is_last == 1)
        def _():
            for h in range(n_head):
                dq_ref[h] = (dq_acc[h].T * scaling).astype(BF16)


def block_call(table, q, do, aug, kv, dq_in, is_end, has_diag, name):
    n_q, n_head, n_row, head_dim = q.shape
    n_key = kv.shape[1]
    n_step = table.shape[0]
    has_in = dq_in is not None
    q_spec = pl.BlockSpec((None, n_head, n_row, head_dim), lambda t, tab: (tab[t, 0], 0, 0, 0))
    qt_spec = pl.BlockSpec((None, n_head, head_dim, n_row), lambda t, tab: (tab[t, 0], 0, 0, 0))
    kv_specs = [pl.BlockSpec((None, None, n_row, head_dim), lambda t, tab, i=i: (i, tab[t, 1], 0, 0)) for i in range(2)]
    n_task = 8 * (n_key // 4)
    return pl.pallas_call(
        functools.partial(block_kernel, has_in, is_end, has_diag),
        grid_spec=pltpu.PrefetchScalarGridSpec(
            num_scalar_prefetch=1,
            grid=(n_step,),
            in_specs=[q_spec, q_spec, q_spec] + kv_specs + ([qt_spec] if has_in else []),
            out_specs=[q_spec if is_end else qt_spec, pl.BlockSpec((2, n_key, head_dim, n_row), lambda t, tab: (0, 0, 0, 0), pipeline_mode=pl.Buffered(1))],
            scratch_shapes=[
                pltpu.VMEM((2 * head_dim, n_row), BF16),
                pltpu.VMEM((2 * head_dim, n_row), BF16),
                pltpu.VMEM((2, Q_TILE, n_row), BF16),
                pltpu.VMEM((2, Q_TILE, n_row), BF16),
            ] + ([pltpu.VMEM((n_head, head_dim, n_row), F32)] if is_end else []),
        ),
        out_shape=[
            jax.ShapeDtypeStruct(q.shape, BF16) if is_end else jax.ShapeDtypeStruct((n_q, n_head, head_dim, n_row), F32),
            jax.ShapeDtypeStruct((2, n_key, head_dim, n_row), F32),
        ],
        compiler_params=pltpu.CompilerParams(dimension_semantics=('arbitrary',), vmem_limit_bytes=40 * 1024 * 1024),
        cost_estimate=pl.CostEstimate(flops=n_task * n_head * 10 * n_row * n_row * head_dim, bytes_accessed=16 * 1024 * 1024, transcendentals=n_task * n_head * n_row * n_row),
        name=name,
    )(table, q, do, aug, kv, kv, *([dq_in] if has_in else []))


def split_parts(x):
    parts = []
    for _ in range(N_PART):
        part = lax.reduce_precision(x, 8, 7)
        parts.append(part)
        x = x - part
    return parts


def solution(mesh):
    n_cx = mesh.shape['cx']
    n_ctx = mesh.shape['cy'] * n_cx
    ctx_axes = ('cy', 'cx')
    row_spec = P(('dp', 'cy', 'cx'), None, None)
    stat_spec = P(('dp', 'cy', 'cx'), None)

    def swap(x, bit):
        return lax.ppermute(x, ctx_axes, [(dev, dev ^ bit) for dev in range(n_ctx)])

    def local_grads(query_rows, key_rows, value_rows, out_rows, grad_out, log_sum_exp):
        tok_dev, n_heads, head_dim = query_rows.shape
        kv_heads = key_rows.shape[1]
        group_size = n_heads // kv_heads
        half_tok = tok_dev // 2
        scaling = 1.0 / math.sqrt(head_dim)
        n_grp = kv_heads // 2
        ctx_rank = lax.axis_index('cy') * n_cx + lax.axis_index('cx')
        core = ctx_rank % 2

        def pick(x, mine):
            sel = core if mine else 1 - core
            return lax.dynamic_slice_in_dim(x, sel * n_grp, n_grp, axis=0)

        def pieces_first(rows):
            return rows.reshape(2, half_tok, kv_heads, group_size, head_dim).transpose(2, 0, 3, 1, 4)

        kv_rows = jnp.stack([key_rows, value_rows]).reshape(2, 2, half_tok, kv_heads, head_dim).transpose(3, 0, 1, 2, 4)
        kv_mine, kv_send = pick(kv_rows, True), pick(kv_rows, False)
        kv_chip = [jnp.concatenate([kv_mine[g], swap(kv_send[g], 1)], axis=1) for g in range(n_grp)]

        q_pf, do_pf = pieces_first(query_rows), pieces_first(grad_out)
        delta = jnp.einsum('thd,thd->th', grad_out, out_rows, preferred_element_type=F32)
        stats = jnp.stack([log_sum_exp * math.sqrt(head_dim), delta])
        stats = stats.reshape(2, 2, half_tok, kv_heads, group_size).transpose(3, 0, 1, 4, 2)

        def chip_rows(x, g, axis=0):
            mine, send = pick(x, True)[g], pick(x, False)[g]
            return jnp.concatenate([mine, swap(send, 1)], axis=axis)

        tables = {name: jnp.asarray(task_table(n_ctx, peers))[ctx_rank] for name, peers in (('own', (0,)), ('far', (3,)), ('near', (1, 2)))}

        def far(g):
            return swap(kv_chip[g], 6)

        def near(g):
            return jnp.concatenate([swap(kv_chip[g], 2), swap(kv_chip[g], 4)], axis=1)

        dq_out, dkv_out = [], []
        kv_far = [far(g) for g in range(n_grp)]
        kv_near = [near(g) for g in range(n_grp)]
        for g in range(n_grp):
            q, do, st = chip_rows(q_pf, g), chip_rows(do_pf, g), chip_rows(stats, g, axis=1)
            parts = jnp.stack(split_parts(st[0]) + split_parts(st[1]), axis=-1).astype(BF16)
            aug = jnp.pad(parts, ((0, 0), (0, 0), (0, 0), (0, 128 - 2 * N_PART)))
            run = functools.partial
            own = lambda dq_in, is_end: block_call(tables['own'], q, do, aug, kv_chip[g], dq_in, is_end, True, 'own_grads')
            farther = lambda dq_in: block_call(tables['far'], q, do, aug, kv_far[g], dq_in, False, False, 'far_grads')
            nearer = lambda dq_in, is_end: block_call(tables['near'], q, do, aug, kv_near[g], dq_in, is_end, False, 'near_grads')
            last = g == n_grp - 1
            dq = None
            if not last:
                dq, dkv_own = own(dq, False)
            dq, dkv_far = farther(dq)
            dq, dkv_near = nearer(dq, not last)
            if last:
                dq, dkv_own = own(dq, True)
            dkv_x, dkv_y = dkv_near[:, :4], dkv_near[:, 4:]
            dkv = dkv_own + swap(dkv_far, 6) + swap(dkv_x, 2) + swap(dkv_y, 4)
            dkv = jnp.stack([dkv[0] * scaling, dkv[1]]).astype(BF16)
            dq_home = jnp.stack([dq[:2], swap(dq[2:], 1)])
            dkv_home = jnp.stack([dkv[:, :2], swap(dkv[:, 2:], 1)])
            dq_out.append(dq_home)
            dkv_out.append(dkv_home)

        def by_core(x):
            return jnp.where(core == 0, x, x[::-1])

        dq_all = by_core(jnp.stack(dq_out, axis=1))
        grad_query = dq_all.transpose(2, 4, 0, 1, 3, 5).reshape(tok_dev, n_heads, head_dim)
        dkv_all = by_core(jnp.stack(dkv_out, axis=1))
        grad_kv = dkv_all.transpose(2, 3, 5, 0, 1, 4).reshape(2, tok_dev, kv_heads, head_dim)
        return grad_query, grad_kv[0], grad_kv[1]

    return jax.shard_map(local_grads, mesh=mesh, in_specs=(row_spec, row_spec, row_spec, row_spec, row_spec, stat_spec), out_specs=(row_spec, row_spec, row_spec), check_vma=False)
```

```python
import functools
import math
import numpy as np
import jax
import jax.numpy as jnp
from jax import lax
from jax.experimental import pallas as pl
from jax.experimental.pallas import tpu as pltpu
from jax.sharding import PartitionSpec as P

LOG2E = math.log2(math.e)
F32 = jnp.float32
BF16 = jnp.bfloat16
Q_TILE = 256


def task_table(n_ctx, peers):
    tables = []
    for rank in range(n_ctx):
        chip, core = rank // 2, rank % 2

        def ids(chip_id):
            devs = (2 * chip_id + core, 2 * chip_id + 1 - core)
            return [dev if half == 0 else 2 * n_ctx - 1 - dev for dev in devs for half in range(2)]

        rows = []
        keys = [piece for peer in peers for piece in ids(chip ^ peer)]
        for q_slot, q_id in enumerate(ids(chip)):
            todo = [(k_slot, 2 if k_id == q_id else 1) for k_slot, k_id in enumerate(keys) if k_id <= q_id]
            todo = todo or [(rows[-1][1] if rows else 0, 0)]
            for n, (k_slot, kind) in enumerate(todo):
                rows.append([q_slot, k_slot, kind, int(n == 0), int(n == len(todo) - 1)])
        tables.append(rows)
    n_step = max(len(rows) for rows in tables)
    for rows in tables:
        while len(rows) < n_step:
            rows.append([rows[-1][0], rows[-1][1], 3, 0, 0])
    return np.array(tables, np.int32)


def block_kernel(has_in, is_end, has_diag, n_peer, tab_ref, q_ref, do_ref, lse_ref, delta_ref, k_ref, v_ref, *refs):
    if has_in:
        dqi_ref, *refs = refs
    dq_ref, *refs = refs
    dkv_refs, (dkv_acc, kt_scr, vt_scr, p_scr, ds_scr, out_sem, *refs) = refs[:n_peer], refs[n_peer:]
    dq_acc = refs[0] if is_end else dq_ref
    n_head, n_row, head_dim = q_ref.shape
    scaling = 1.0 / math.sqrt(head_dim)
    step = pl.program_id(0)
    k_slot = tab_ref[step, 1]
    kind = tab_ref[step, 2]
    is_first = tab_ref[step, 3]
    is_last = tab_ref[step, 4]
    n_sub = n_row // Q_TILE

    @pl.when(step == 0)
    def _():
        dkv_acc[...] = jnp.zeros_like(dkv_acc)

    def run_task(masked):
        kt_scr[...] = k_ref[...].T
        vt_scr[...] = v_ref[...].T
        fresh = is_first == 1

        def scores(h, sub, slot):
            rows = pl.ds(sub * Q_TILE, Q_TILE)
            n_key = n_row if not masked else (sub + 1) * Q_TILE
            s = jnp.dot(q_ref[h, rows, :], kt_scr[:, :n_key], preferred_element_type=F32)
            dp = jnp.dot(do_ref[h, rows, :], vt_scr[:, :n_key], preferred_element_type=F32)
            lse = jnp.tile(lse_ref[h, rows, :], (1, n_key // 128))
            dlt = jnp.tile(delta_ref[h, rows, :], (1, n_key // 128))
            prob = jnp.exp2(s * (scaling * LOG2E) - lse)
            if masked:
                qi = lax.broadcasted_iota(jnp.int32, s.shape, 0) + sub * Q_TILE
                kj = lax.broadcasted_iota(jnp.int32, s.shape, 1)
                prob = jnp.where(qi >= kj, prob, 0.0)
            p_scr[slot, :, :n_key] = prob.astype(BF16)
            ds_scr[slot, :, :n_key] = (prob * (dp - dlt)).astype(BF16)

        def grads(h, sub, slot):
            rows = pl.ds(sub * Q_TILE, Q_TILE)
            n_key = n_row if not masked else (sub + 1) * Q_TILE
            prob = p_scr[slot, :, :n_key]
            ds = ds_scr[slot, :, :n_key]
            dkv_acc[k_slot, 1, :, :n_key] += lax.dot_general(do_ref[h, rows, :], prob, (((0,), (0,)), ((), ())), preferred_element_type=F32)
            dkv_acc[k_slot, 0, :, :n_key] += lax.dot_general(q_ref[h, rows, :], ds, (((0,), (0,)), ((), ())), preferred_element_type=F32)
            base = jnp.where(fresh, dqi_ref[h, rows, :] if has_in else 0.0, dq_acc[h, rows, :])
            dq_acc[h, rows, :] = base + jnp.dot(ds, k_ref[:n_key, :], preferred_element_type=F32)

        tiles = [(h, sub) for h in range(n_head) for sub in range(n_sub)]
        scores(*tiles[0], 0)
        for idx, tile in enumerate(tiles):
            if idx + 1 < len(tiles):
                scores(*tiles[idx + 1], (idx + 1) % 2)
            grads(*tile, idx % 2)

    @pl.when(kind == 1)
    def _():
        run_task(False)

    if has_diag:
        @pl.when(kind == 2)
        def _():
            run_task(True)
    else:
        @pl.when(kind == 0)
        def _():
            dq_acc[...] = dqi_ref[...] if has_in else jnp.zeros_like(dq_acc)

    if is_end:
        @pl.when(is_last == 1)
        def _():
            dq_ref[...] = (dq_acc[...] * scaling).astype(BF16)

    @pl.when(step == pl.num_programs(0) - 1)
    def _():
        copies = [pltpu.make_async_copy(dkv_acc.at[pl.ds(4 * i, 4)], dkv_refs[i], out_sem.at[i]) for i in range(n_peer)]
        for copy in copies:
            copy.start()
        for copy in copies:
            copy.wait()


def block_call(table, q, do, lse, delta, kv, dq_in, is_end, has_diag):
    _, n_head, n_row, head_dim = q.shape
    n_key = kv.shape[1]
    n_peer = n_key // 4
    n_step = table.shape[0]
    has_in = dq_in is not None
    q_spec = pl.BlockSpec((None, n_head, n_row, head_dim), lambda t, tab: (tab[t, 0], 0, 0, 0))
    kv_specs = [pl.BlockSpec((None, None, n_row, head_dim), lambda t, tab, i=i: (i, tab[t, 1], 0, 0)) for i in range(2)]
    n_task = 8 * n_peer
    return pl.pallas_call(
        functools.partial(block_kernel, has_in, is_end, has_diag, n_peer),
        grid_spec=pltpu.PrefetchScalarGridSpec(
            num_scalar_prefetch=1,
            grid=(n_step,),
            in_specs=[q_spec] * 4 + kv_specs + ([q_spec] if has_in else []),
            out_specs=[q_spec] + [pl.BlockSpec(memory_space=pl.ANY)] * n_peer,
            scratch_shapes=[
                pltpu.VMEM((n_key, 2, head_dim, n_row), F32),
                pltpu.VMEM((head_dim, n_row), BF16),
                pltpu.VMEM((head_dim, n_row), BF16),
                pltpu.VMEM((2, Q_TILE, n_row), BF16),
                pltpu.VMEM((2, Q_TILE, n_row), BF16),
                pltpu.SemaphoreType.DMA((n_peer,)),
            ] + ([pltpu.VMEM((n_head, n_row, head_dim), F32)] if is_end else []),
        ),
        out_shape=[jax.ShapeDtypeStruct(q.shape, BF16 if is_end else F32)] + [jax.ShapeDtypeStruct((4, 2, head_dim, n_row), F32)] * n_peer,
        compiler_params=pltpu.CompilerParams(dimension_semantics=('arbitrary',), vmem_limit_bytes=48 * 1024 * 1024),
        cost_estimate=pl.CostEstimate(flops=n_task * n_head * 10 * n_row * n_row * head_dim, bytes_accessed=32 * 1024 * 1024, transcendentals=n_task * n_head * n_row * n_row),
    )(table, q, do, lse, delta, kv, kv, *([dq_in] if has_in else []))


def solution(mesh):
    n_cx = mesh.shape['cx']
    n_ctx = mesh.shape['cy'] * n_cx
    ctx_axes = ('cy', 'cx')
    row_spec = P(('dp', 'cy', 'cx'), None, None)
    stat_spec = P(('dp', 'cy', 'cx'), None)

    def swap(x, bit):
        return lax.ppermute(x, ctx_axes, [(dev, dev ^ bit) for dev in range(n_ctx)])

    def local_grads(query_rows, key_rows, value_rows, out_rows, grad_out, log_sum_exp):
        tok_dev, n_heads, head_dim = query_rows.shape
        kv_heads = key_rows.shape[1]
        group_size = n_heads // kv_heads
        half_tok = tok_dev // 2
        scaling = 1.0 / math.sqrt(head_dim)
        n_grp = kv_heads // 2
        ctx_rank = lax.axis_index('cy') * n_cx + lax.axis_index('cx')
        core = ctx_rank % 2

        def pick(x, g, mine):
            sel = core if mine else 1 - core
            return lax.dynamic_index_in_dim(x, sel * n_grp + g, axis=0, keepdims=False)

        def pieces_first(rows):
            return rows.reshape(2, half_tok, kv_heads, group_size, head_dim).transpose(2, 0, 3, 1, 4)

        def chip_rows(x, g, axis=0):
            return jnp.concatenate([pick(x, g, True), swap(pick(x, g, False), 1)], axis=axis)

        kv_rows = jnp.stack([key_rows, value_rows]).reshape(2, 2, half_tok, kv_heads, head_dim).transpose(3, 0, 1, 2, 4)
        kv_chip = [chip_rows(kv_rows, g, axis=1) for g in range(n_grp)]
        kv_far = [swap(kv_chip[g], 6) for g in range(n_grp)]
        kv_near = [jnp.concatenate([swap(kv_chip[g], 2), swap(kv_chip[g], 4)], axis=1) for g in range(n_grp)]

        q_pf, do_pf = pieces_first(query_rows), pieces_first(grad_out)
        q_pf, do_pf = lax.optimization_barrier((q_pf, do_pf))
        delta = jnp.einsum('thd,thd->th', grad_out, out_rows, preferred_element_type=F32)

        def stat_first(stat):
            return stat.reshape(2, half_tok, kv_heads, group_size).transpose(2, 0, 3, 1)

        stats = jnp.stack([stat_first(log_sum_exp * LOG2E), stat_first(delta)], axis=1)
        tables = {name: jnp.asarray(task_table(n_ctx, peers))[ctx_rank] for name, peers in (('own', (0,)), ('far', (3,)), ('near', (1, 2)))}

        def lanes(stat):
            return jnp.broadcast_to(stat[..., None], stat.shape + (128,))

        dq_all = jnp.zeros((kv_heads, 2, group_size, half_tok, head_dim), BF16)
        dkv_all = jnp.zeros((kv_heads, 2, 2, head_dim, half_tok), BF16)
        for g in range(n_grp):
            q = chip_rows(q_pf, g)
            do = chip_rows(do_pf, g)
            stat = chip_rows(stats, g, axis=1)
            rows = (q, do, lanes(stat[0]), lanes(stat[1]))

            def run(kind, kv, dq_in, is_end):
                return block_call(tables[kind], *rows, kv, dq_in, is_end, kind == 'own')

            last = g == n_grp - 1
            dq = None
            if not last:
                dq, dkv_own = run('own', kv_chip[g], None, False)
            dq, dkv_far = run('far', kv_far[g], dq, False)
            dq, dkv_x, dkv_y = run('near', kv_near[g], dq, not last)
            if last:
                dq, dkv_own = run('own', kv_chip[g], dq, True)
            dkv = dkv_own + swap(dkv_far, 6) + swap(dkv_x, 2) + swap(dkv_y, 4)
            dkv = (dkv * jnp.array([scaling, 1.0], F32)[None, :, None, None]).astype(BF16)
            dq_all = lax.dynamic_update_index_in_dim(dq_all, dq[:2], core * n_grp + g, 0)
            dq_all = lax.dynamic_update_index_in_dim(dq_all, swap(dq[2:], 1), (1 - core) * n_grp + g, 0)
            dkv_all = lax.dynamic_update_index_in_dim(dkv_all, dkv[:2], core * n_grp + g, 0)
            dkv_all = lax.dynamic_update_index_in_dim(dkv_all, swap(dkv[2:], 1), (1 - core) * n_grp + g, 0)

        grad_query = dq_all.transpose(1, 3, 0, 2, 4).reshape(tok_dev, n_heads, head_dim)
        grad_kv = dkv_all.transpose(2, 1, 4, 0, 3).reshape(2, tok_dev, kv_heads, head_dim)
        return grad_query, grad_kv[0], grad_kv[1]

    return jax.shard_map(local_grads, mesh=mesh, in_specs=(row_spec, row_spec, row_spec, row_spec, row_spec, stat_spec), out_specs=(row_spec, row_spec, row_spec), check_vma=False)
```

```python
import functools
import math
import numpy as np
import jax
import jax.numpy as jnp
from jax import lax
from jax.experimental import pallas as pl
from jax.experimental.pallas import tpu as pltpu
from jax.sharding import PartitionSpec as P

LOG2E = math.log2(math.e)
F32 = jnp.float32
BF16 = jnp.bfloat16
Q_TILE = 256
FULL_TILE = 512
N_PART = 3


def task_table(n_ctx, peers):
    tables = []
    for rank in range(n_ctx):
        chip, core = rank // 2, rank % 2

        def ids(chip_id):
            devs = (2 * chip_id + core, 2 * chip_id + 1 - core)
            return [dev if half == 0 else 2 * n_ctx - 1 - dev for dev in devs for half in range(2)]

        rows = []
        keys = [piece for peer in peers for piece in ids(chip ^ peer)]
        for q_slot, q_id in enumerate(ids(chip)):
            todo = [(k_slot, 2 if k_id == q_id else 1) for k_slot, k_id in enumerate(keys) if k_id <= q_id]
            todo = todo or [(rows[-1][1] if rows else 0, 0)]
            for n, (k_slot, kind) in enumerate(todo):
                rows.append([q_slot, k_slot, kind, int(n == 0), int(n == len(todo) - 1)])
        tables.append(rows)
    n_step = max(len(rows) for rows in tables)
    for rows in tables:
        while len(rows) < n_step:
            rows.append([rows[-1][0], rows[-1][1], 3, 0, 0])
    return np.array(tables, np.int32)


def block_kernel(has_in, is_end, has_diag, n_peer, tab_ref, q_ref, do_ref, aug_ref, k_ref, v_ref, *refs):
    if has_in:
        dqi_ref, *refs = refs
    dq_ref, *refs = refs
    dkv_refs, (dkv_acc, kt_scr, vt_scr, p_scr, ds_scr, dkv_rows, out_sem, *refs) = refs[:n_peer], refs[n_peer:]
    dq_acc = refs[0] if is_end else dq_ref
    n_head, n_row, head_dim = q_ref.shape
    scaling = 1.0 / math.sqrt(head_dim)
    step = pl.program_id(0)
    k_slot = tab_ref[step, 1]
    kind = tab_ref[step, 2]
    is_first = tab_ref[step, 3]
    is_last = tab_ref[step, 4]

    @pl.when(step == 0)
    def _():
        dkv_acc[...] = jnp.zeros_like(dkv_acc)
        row_id = lax.broadcasted_iota(jnp.int32, (head_dim, n_row), 0)
        kt_scr[head_dim:, :] = jnp.where(row_id < N_PART, -1.0, 0.0).astype(BF16)
        vt_scr[head_dim:, :] = jnp.where((row_id >= N_PART) & (row_id < 2 * N_PART), -1.0, 0.0).astype(BF16)

    if has_in:
        @pl.when(is_first == 1)
        def _():
            dq_acc[...] = dqi_ref[...]

    def run_task(masked):
        tile = Q_TILE if masked else FULL_TILE
        kt_scr[:head_dim, :] = k_ref[...].T
        vt_scr[:head_dim, :] = v_ref[...].T
        fresh = is_first == 1

        def scores(h, sub, slot):
            rows = pl.ds(sub * tile, tile)
            n_key = n_row if not masked else (sub + 1) * tile
            aug = aug_ref[h, rows, :]
            s = jnp.dot(jnp.concatenate([q_ref[h, rows, :], aug], axis=1), kt_scr[:, :n_key], preferred_element_type=F32)
            dp = jnp.dot(jnp.concatenate([do_ref[h, rows, :], aug], axis=1), vt_scr[:, :n_key], preferred_element_type=F32)
            prob = jnp.exp2(s * (scaling * LOG2E))
            if masked:
                qi = lax.broadcasted_iota(jnp.int32, s.shape, 0) + sub * tile
                kj = lax.broadcasted_iota(jnp.int32, s.shape, 1)
                prob = jnp.where(qi >= kj, prob, 0.0)
            p_scr[slot, :tile, :n_key] = prob.astype(BF16)
            ds_scr[slot, :tile, :n_key] = (prob * dp).astype(BF16)

        def grads(h, sub, slot):
            rows = pl.ds(sub * tile, tile)
            n_key = n_row if not masked else (sub + 1) * tile
            prob = p_scr[slot, :tile, :n_key]
            ds = ds_scr[slot, :tile, :n_key]
            dkv_acc[k_slot, 1, :, :n_key] += lax.dot_general(do_ref[h, rows, :], prob, (((0,), (0,)), ((), ())), preferred_element_type=F32)
            dkv_acc[k_slot, 0, :, :n_key] += lax.dot_general(q_ref[h, rows, :], ds, (((0,), (0,)), ((), ())), preferred_element_type=F32)
            base = dq_acc[h, :, rows] if has_in else jnp.where(fresh, 0.0, dq_acc[h, :, rows])
            dq_acc[h, :, rows] = base + lax.dot_general(kt_scr[:head_dim, :n_key], ds, (((1,), (1,)), ((), ())), preferred_element_type=F32)

        tiles = [(h, sub) for h in range(n_head) for sub in range(n_row // tile)]
        scores(*tiles[0], 0)
        for idx, tile_id in enumerate(tiles):
            if idx + 1 < len(tiles):
                scores(*tiles[idx + 1], (idx + 1) % 2)
            grads(*tile_id, idx % 2)

    @pl.when(kind == 1)
    def _():
        run_task(False)

    if has_diag:
        @pl.when(kind == 2)
        def _():
            run_task(True)
    elif not has_in:
        @pl.when(kind == 0)
        def _():
            dq_acc[...] = jnp.zeros_like(dq_acc)

    if is_end:
        @pl.when(is_last == 1)
        def _():
            for h in range(n_head):
                dq_ref[h] = (dq_acc[h].T * scaling).astype(BF16)

    @pl.when(step == pl.num_programs(0) - 1)
    def _():
        for i in range(n_peer):
            @pl.loop(0, 4)
            def _(j):
                dkv_rows[i, 0, j] = dkv_acc[4 * i + j, 0].T * scaling
                dkv_rows[i, 1, j] = dkv_acc[4 * i + j, 1].T

            pltpu.make_async_copy(dkv_rows.at[i], dkv_refs[i], out_sem.at[i]).start()
        for i in range(n_peer):
            pltpu.make_async_copy(dkv_rows.at[i], dkv_refs[i], out_sem.at[i]).wait()


def block_call(table, q, do, aug, kv, dq_in, is_end, has_diag):
    n_q, n_head, n_row, head_dim = q.shape
    n_key = kv.shape[1]
    n_peer = n_key // 4
    n_step = table.shape[0]
    has_in = dq_in is not None
    q_spec = pl.BlockSpec((None, n_head, n_row, head_dim), lambda t, tab: (tab[t, 0], 0, 0, 0))
    kv_specs = [pl.BlockSpec((None, None, n_row, head_dim), lambda t, tab, i=i: (i, tab[t, 1], 0, 0)) for i in range(2)]
    qt_spec = pl.BlockSpec((None, n_head, head_dim, n_row), lambda t, tab: (tab[t, 0], 0, 0, 0))
    n_task = 8 * n_peer
    return pl.pallas_call(
        functools.partial(block_kernel, has_in, is_end, has_diag, n_peer),
        grid_spec=pltpu.PrefetchScalarGridSpec(
            num_scalar_prefetch=1,
            grid=(n_step,),
            in_specs=[q_spec] * 3 + kv_specs + ([qt_spec] if has_in else []),
            out_specs=[q_spec if is_end else qt_spec] + [pl.BlockSpec(memory_space=pl.ANY)] * n_peer,
            scratch_shapes=[
                pltpu.VMEM((n_key, 2, head_dim, n_row), F32),
                pltpu.VMEM((2 * head_dim, n_row), BF16),
                pltpu.VMEM((2 * head_dim, n_row), BF16),
                pltpu.VMEM((2, FULL_TILE, n_row), BF16),
                pltpu.VMEM((2, FULL_TILE, n_row), BF16),
                pltpu.VMEM((n_peer, 2, 4, n_row, head_dim), F32),
                pltpu.SemaphoreType.DMA((n_peer,)),
            ] + ([pltpu.VMEM((n_head, head_dim, n_row), F32)] if is_end else []),
        ),
        out_shape=[jax.ShapeDtypeStruct(q.shape, BF16) if is_end else jax.ShapeDtypeStruct((n_q, n_head, head_dim, n_row), F32)] + [jax.ShapeDtypeStruct((2, 4, n_row, head_dim), F32)] * n_peer,
        compiler_params=pltpu.CompilerParams(dimension_semantics=('arbitrary',), vmem_limit_bytes=50 * 1024 * 1024),
        cost_estimate=pl.CostEstimate(flops=n_task * n_head * 10 * n_row * n_row * head_dim, bytes_accessed=32 * 1024 * 1024, transcendentals=n_task * n_head * n_row * n_row),
    )(table, q, do, aug, kv, kv, *([dq_in] if has_in else []))


def lane_parts(lse, delta):
    lane = lax.broadcasted_iota(jnp.int32, lse.shape + (128,), lse.ndim)
    rest = jnp.where(lane < N_PART, lse[..., None], delta[..., None])
    part = lax.reduce_precision(rest, 8, 7)
    out = part
    for n in range(1, N_PART):
        rest = rest - part
        part = lax.reduce_precision(rest, 8, 7)
        out = jnp.where(lane % N_PART == n, part, out)
    return jnp.where(lane < 2 * N_PART, out, 0.0).astype(BF16)


def solution(mesh):
    n_cx = mesh.shape['cx']
    n_ctx = mesh.shape['cy'] * n_cx
    ctx_axes = ('cy', 'cx')
    row_spec = P(('dp', 'cy', 'cx'), None, None)
    stat_spec = P(('dp', 'cy', 'cx'), None)

    def swap(x, bit):
        return lax.ppermute(x, ctx_axes, [(dev, dev ^ bit) for dev in range(n_ctx)])

    def local_grads(query_rows, key_rows, value_rows, out_rows, grad_out, log_sum_exp):
        tok_dev, n_heads, head_dim = query_rows.shape
        kv_heads = key_rows.shape[1]
        group_size = n_heads // kv_heads
        half_tok = tok_dev // 2
        n_grp = kv_heads // 2
        ctx_rank = lax.axis_index('cy') * n_cx + lax.axis_index('cx')
        core = ctx_rank % 2

        def pick(x, g, mine):
            sel = core if mine else 1 - core
            return lax.dynamic_index_in_dim(x, sel * n_grp + g, axis=0, keepdims=False)

        def pieces_first(rows):
            return rows.reshape(2, half_tok, kv_heads, group_size, head_dim).transpose(2, 0, 3, 1, 4)

        def chip_rows(x, g, axis=0):
            return jnp.concatenate([pick(x, g, True), swap(pick(x, g, False), 1)], axis=axis)

        kv_rows = jnp.stack([key_rows, value_rows]).reshape(2, 2, half_tok, kv_heads, head_dim).transpose(3, 0, 1, 2, 4)
        kv_chip = [chip_rows(kv_rows, g, axis=1) for g in range(n_grp)]
        kv_far = [swap(kv_chip[g], 6) for g in range(n_grp)]
        kv_near = [jnp.concatenate([swap(kv_chip[g], 2), swap(kv_chip[g], 4)], axis=1) for g in range(n_grp)]

        q_pf, do_pf = pieces_first(query_rows), pieces_first(grad_out)
        q_pf, do_pf = lax.optimization_barrier((q_pf, do_pf))
        delta = jnp.einsum('thd,thd->th', grad_out, out_rows, preferred_element_type=F32)

        def stat_first(stat):
            return stat.reshape(2, half_tok, kv_heads, group_size).transpose(2, 0, 3, 1)

        stats = jnp.stack([stat_first(log_sum_exp * math.sqrt(head_dim)), stat_first(delta)], axis=1)
        tables = {name: jnp.asarray(task_table(n_ctx, peers))[ctx_rank] for name, peers in (('own', (0,)), ('far', (3,)), ('near', (1, 2)))}

        dq_all, dkv_all = q_pf, kv_rows
        for g in range(n_grp):
            q = chip_rows(q_pf, g)
            do = chip_rows(do_pf, g)
            stat = chip_rows(stats, g, axis=1)
            rows = (q, do, lane_parts(stat[0], stat[1]))

            def run(kind, kv, dq_in, is_end):
                return block_call(tables[kind], *rows, kv, dq_in, is_end, kind == 'own')

            last = g == n_grp - 1
            dq = None
            if not last:
                dq, dkv_own = run('own', kv_chip[g], None, False)
            dq, dkv_far = run('far', kv_far[g], dq, False)
            dq, dkv_x, dkv_y = run('near', kv_near[g], dq, not last)
            if last:
                dq, dkv_own = run('own', kv_chip[g], dq, True)
            dkv = dkv_own + swap(dkv_far, 6) + swap(dkv_x, 2) + swap(dkv_y, 4)
            dkv = dkv.astype(BF16)
            dq_all = lax.dynamic_update_index_in_dim(dq_all, dq[:2], core * n_grp + g, 0)
            dq_all = lax.dynamic_update_index_in_dim(dq_all, swap(dq[2:], 1), (1 - core) * n_grp + g, 0)
            dkv_all = lax.dynamic_update_index_in_dim(dkv_all, dkv[:, :2], core * n_grp + g, 0)
            dkv_all = lax.dynamic_update_index_in_dim(dkv_all, swap(dkv[:, 2:], 1), (1 - core) * n_grp + g, 0)

        grad_query = dq_all.transpose(1, 3, 0, 2, 4).reshape(tok_dev, n_heads, head_dim)
        grad_kv = dkv_all.transpose(1, 2, 3, 0, 4).reshape(2, tok_dev, kv_heads, head_dim)
        return grad_query, grad_kv[0], grad_kv[1]

    return jax.shard_map(local_grads, mesh=mesh, in_specs=(row_spec, row_spec, row_spec, row_spec, row_spec, stat_spec), out_specs=(row_spec, row_spec, row_spec), check_vma=False)
```

```python
import functools
import math
import numpy as np
import jax
import jax.numpy as jnp
from jax import lax
from jax.experimental import pallas as pl
from jax.experimental.pallas import tpu as pltpu
from jax.sharding import PartitionSpec as P

LOG2E = math.log2(math.e)
F32 = jnp.float32
BF16 = jnp.bfloat16
Q_TILE = 256
FULL_TILE = 256
N_PART = 3


def task_table(n_ctx, peers):
    tables = []
    for rank in range(n_ctx):
        chip, core = rank // 2, rank % 2

        def ids(chip_id):
            devs = (2 * chip_id + core, 2 * chip_id + 1 - core)
            return [dev if half == 0 else 2 * n_ctx - 1 - dev for dev in devs for half in range(2)]

        rows = []
        keys = [piece for peer in peers for piece in ids(chip ^ peer)]
        for q_slot, q_id in enumerate(ids(chip)):
            todo = [(k_slot, 2 if k_id == q_id else 1) for k_slot, k_id in enumerate(keys) if k_id <= q_id]
            todo = todo or [(rows[-1][1] if rows else 0, 0)]
            for n, (k_slot, kind) in enumerate(todo):
                rows.append([q_slot, k_slot, kind, int(n == 0), int(n == len(todo) - 1)])
        tables.append(rows)
    n_step = max(len(rows) for rows in tables)
    for rows in tables:
        while len(rows) < n_step:
            rows.append([rows[-1][0], rows[-1][1], 3, 0, 0])
    return np.array(tables, np.int32)


def block_kernel(has_in, is_end, has_diag, n_peer, tab_ref, q_ref, do_ref, aug_ref, *refs):
    kv_refs, refs = refs[:2 * n_peer], refs[2 * n_peer:]
    if has_in:
        dqi_ref, *refs = refs
    dq_ref, *refs = refs
    dkv_refs, (dkv_acc, kt_scr, vt_scr, p_scr, ds_scr, dkv_rows, out_sem, *refs) = refs[:n_peer], refs[n_peer:]
    dq_acc = refs[0] if is_end else dq_ref
    n_head, n_row, head_dim = q_ref.shape
    scaling = 1.0 / math.sqrt(head_dim)
    step = pl.program_id(0)
    k_slot = tab_ref[step, 1]
    kind = tab_ref[step, 2]
    is_first = tab_ref[step, 3]
    is_last = tab_ref[step, 4]

    @pl.when(step == 0)
    def _():
        dkv_acc[...] = jnp.zeros_like(dkv_acc)
        row_id = lax.broadcasted_iota(jnp.int32, (head_dim, n_row), 0)
        kt_scr[head_dim:, :] = jnp.where(row_id < N_PART, -1.0, 0.0).astype(BF16)
        vt_scr[head_dim:, :] = jnp.where((row_id >= N_PART) & (row_id < 2 * N_PART), -1.0, 0.0).astype(BF16)

    def run_task(masked):
        tile = Q_TILE if masked else FULL_TILE
        k_blk, v_blk = kv_refs[0][...], kv_refs[1][...]
        if n_peer == 2:
            k_blk = jnp.where(k_slot < 4, k_blk, kv_refs[2][...])
            v_blk = jnp.where(k_slot < 4, v_blk, kv_refs[3][...])
        kt_scr[:head_dim, :] = k_blk.T
        vt_scr[:head_dim, :] = v_blk.T
        fresh = is_first == 1

        def scores(h, sub, slot):
            rows = pl.ds(sub * tile, tile)
            n_key = n_row if not masked else (sub + 1) * tile
            aug = aug_ref[h, rows, :]
            s = jnp.dot(jnp.concatenate([q_ref[h, rows, :], aug], axis=1), kt_scr[:, :n_key], preferred_element_type=F32)
            dp = jnp.dot(jnp.concatenate([do_ref[h, rows, :], aug], axis=1), vt_scr[:, :n_key], preferred_element_type=F32)
            prob = jnp.exp2(s * (scaling * LOG2E))
            if masked:
                qi = lax.broadcasted_iota(jnp.int32, s.shape, 0) + sub * tile
                kj = lax.broadcasted_iota(jnp.int32, s.shape, 1)
                prob = jnp.where(qi >= kj, prob, 0.0)
            p_scr[slot, :tile, :n_key] = prob.astype(BF16)
            ds_scr[slot, :tile, :n_key] = (prob * dp).astype(BF16)

        def grads(h, sub, slot):
            rows = pl.ds(sub * tile, tile)
            n_key = n_row if not masked else (sub + 1) * tile
            prob = p_scr[slot, :tile, :n_key]
            ds = ds_scr[slot, :tile, :n_key]
            dkv_acc[k_slot, 1, :, :n_key] += lax.dot_general(do_ref[h, rows, :], prob, (((0,), (0,)), ((), ())), preferred_element_type=F32)
            dkv_acc[k_slot, 0, :, :n_key] += lax.dot_general(q_ref[h, rows, :], ds, (((0,), (0,)), ((), ())), preferred_element_type=F32)
            base = jnp.where(fresh, dqi_ref[h, :, rows] if has_in else 0.0, dq_acc[h, :, rows])
            dq_acc[h, :, rows] = base + lax.dot_general(kt_scr[:head_dim, :n_key], ds, (((1,), (1,)), ((), ())), preferred_element_type=F32)

        tiles = [(h, sub) for h in range(n_head) for sub in range(n_row // tile)]
        scores(*tiles[0], 0)
        for idx, tile_id in enumerate(tiles):
            if idx + 1 < len(tiles):
                scores(*tiles[idx + 1], (idx + 1) % 2)
            grads(*tile_id, idx % 2)

    @pl.when(kind == 1)
    def _():
        run_task(False)

    if has_diag:
        @pl.when(kind == 2)
        def _():
            run_task(True)
    else:
        @pl.when(kind == 0)
        def _():
            dq_acc[...] = dqi_ref[...] if has_in else jnp.zeros_like(dq_acc)

    if is_end:
        @pl.when(is_last == 1)
        def _():
            for h in range(n_head):
                dq_ref[h] = (dq_acc[h].T * scaling).astype(BF16)

    @pl.when(step == pl.num_programs(0) - 1)
    def _():
        for i in range(n_peer):
            @pl.loop(0, 4)
            def _(j):
                dkv_rows[i, 0, j] = dkv_acc[4 * i + j, 0].T * scaling
                dkv_rows[i, 1, j] = dkv_acc[4 * i + j, 1].T

            pltpu.make_async_copy(dkv_rows.at[i], dkv_refs[i], out_sem.at[i]).start()
        for i in range(n_peer):
            pltpu.make_async_copy(dkv_rows.at[i], dkv_refs[i], out_sem.at[i]).wait()


def block_call(table, q, do, aug, kv, dq_in, is_end, has_diag):
    n_q, n_head, n_row, head_dim = q.shape
    n_peer = len(kv)
    n_key = 4 * n_peer
    n_step = table.shape[0]
    has_in = dq_in is not None
    q_spec = pl.BlockSpec((None, n_head, n_row, head_dim), lambda t, tab: (tab[t, 0], 0, 0, 0))
    kv_specs = [pl.BlockSpec((None, None, n_row, head_dim), lambda t, tab, i=i, p=p: (i, jnp.clip(tab[t, 1] - 4 * p, 0, 3), 0, 0)) for p in range(n_peer) for i in range(2)]
    qt_spec = pl.BlockSpec((None, n_head, head_dim, n_row), lambda t, tab: (tab[t, 0], 0, 0, 0))
    n_task = 8 * n_peer
    return pl.pallas_call(
        functools.partial(block_kernel, has_in, is_end, has_diag, n_peer),
        grid_spec=pltpu.PrefetchScalarGridSpec(
            num_scalar_prefetch=1,
            grid=(n_step,),
            in_specs=[q_spec] * 3 + kv_specs + ([qt_spec] if has_in else []),
            out_specs=[q_spec if is_end else qt_spec] + [pl.BlockSpec(memory_space=pl.ANY)] * n_peer,
            scratch_shapes=[
                pltpu.VMEM((n_key, 2, head_dim, n_row), F32),
                pltpu.VMEM((2 * head_dim, n_row), BF16),
                pltpu.VMEM((2 * head_dim, n_row), BF16),
                pltpu.VMEM((2, FULL_TILE, n_row), BF16),
                pltpu.VMEM((2, FULL_TILE, n_row), BF16),
                pltpu.VMEM((n_peer, 2, 4, n_row, head_dim), F32),
                pltpu.SemaphoreType.DMA((n_peer,)),
            ] + ([pltpu.VMEM((n_head, head_dim, n_row), F32)] if is_end else []),
        ),
        out_shape=[jax.ShapeDtypeStruct(q.shape, BF16) if is_end else jax.ShapeDtypeStruct((n_q, n_head, head_dim, n_row), F32)] + [jax.ShapeDtypeStruct((2, 4, n_row, head_dim), F32)] * n_peer,
        compiler_params=pltpu.CompilerParams(dimension_semantics=('arbitrary',), vmem_limit_bytes=50 * 1024 * 1024),
        cost_estimate=pl.CostEstimate(flops=n_task * n_head * 10 * n_row * n_row * head_dim, bytes_accessed=32 * 1024 * 1024, transcendentals=n_task * n_head * n_row * n_row),
    )(table, q, do, aug, *[x for x in kv for _ in range(2)], *([dq_in] if has_in else []))


def lane_parts(lse, delta):
    lane = lax.broadcasted_iota(jnp.int32, lse.shape + (128,), lse.ndim)
    rest = jnp.where(lane < N_PART, lse[..., None], delta[..., None])
    part = lax.reduce_precision(rest, 8, 7)
    out = part
    for n in range(1, N_PART):
        rest = rest - part
        part = lax.reduce_precision(rest, 8, 7)
        out = jnp.where(lane % N_PART == n, part, out)
    return jnp.where(lane < 2 * N_PART, out, 0.0).astype(BF16)


def solution(mesh):
    n_cx = mesh.shape['cx']
    n_ctx = mesh.shape['cy'] * n_cx
    ctx_axes = ('cy', 'cx')
    row_spec = P(('dp', 'cy', 'cx'), None, None)
    stat_spec = P(('dp', 'cy', 'cx'), None)

    def swap(x, bit):
        return lax.ppermute(x, ctx_axes, [(dev, dev ^ bit) for dev in range(n_ctx)])

    def local_grads(query_rows, key_rows, value_rows, out_rows, grad_out, log_sum_exp):
        tok_dev, n_heads, head_dim = query_rows.shape
        kv_heads = key_rows.shape[1]
        group_size = n_heads // kv_heads
        half_tok = tok_dev // 2
        n_grp = kv_heads // 2
        ctx_rank = lax.axis_index('cy') * n_cx + lax.axis_index('cx')
        core = ctx_rank % 2

        def pick(x, g, mine):
            sel = core if mine else 1 - core
            return lax.dynamic_index_in_dim(x, sel * n_grp + g, axis=0, keepdims=False)

        def pieces_first(rows):
            return rows.reshape(2, half_tok, kv_heads, group_size, head_dim).transpose(2, 0, 3, 1, 4)

        def chip_rows(x, g, axis=0):
            return jnp.concatenate([pick(x, g, True), swap(pick(x, g, False), 1)], axis=axis)

        kv_rows = jnp.stack([key_rows, value_rows]).reshape(2, 2, half_tok, kv_heads, head_dim).transpose(3, 0, 1, 2, 4)
        kv_chip = [chip_rows(kv_rows, g, axis=1) for g in range(n_grp)]
        kv_far = [swap(kv_chip[g], 6) for g in range(n_grp)]
        kv_near = [(swap(kv_chip[g], 2), swap(kv_chip[g], 4)) for g in range(n_grp)]

        q_pf, do_pf = pieces_first(query_rows), pieces_first(grad_out)
        q_pf, do_pf = lax.optimization_barrier((q_pf, do_pf))
        delta = jnp.einsum('thd,thd->th', grad_out, out_rows, preferred_element_type=F32)

        def stat_first(stat):
            return stat.reshape(2, half_tok, kv_heads, group_size).transpose(2, 0, 3, 1)

        stats = jnp.stack([stat_first(log_sum_exp * math.sqrt(head_dim)), stat_first(delta)], axis=1)
        tables = {name: jnp.asarray(task_table(n_ctx, peers))[ctx_rank] for name, peers in (('own', (0,)), ('far', (3,)), ('near', (1, 2)))}

        dq_all, dkv_all = q_pf, kv_rows
        for g in range(n_grp):
            q = chip_rows(q_pf, g)
            do = chip_rows(do_pf, g)
            stat = chip_rows(stats, g, axis=1)
            rows = (q, do, lane_parts(stat[0], stat[1]))

            def run(kind, kv, dq_in, is_end):
                return block_call(tables[kind], *rows, kv, dq_in, is_end, kind == 'own')

            last = g == n_grp - 1
            dq = None
            if not last:
                dq, dkv_own = run('own', (kv_chip[g],), None, False)
            dq, dkv_far = run('far', (kv_far[g],), dq, False)
            dq, dkv_x, dkv_y = run('near', kv_near[g], dq, not last)
            if last:
                dq, dkv_own = run('own', (kv_chip[g],), dq, True)
            dkv = dkv_own + swap(dkv_far, 6) + swap(dkv_x, 2) + swap(dkv_y, 4)
            dkv = dkv.astype(BF16)
            dq_all = lax.dynamic_update_index_in_dim(dq_all, dq[:2], core * n_grp + g, 0)
            dq_all = lax.dynamic_update_index_in_dim(dq_all, swap(dq[2:], 1), (1 - core) * n_grp + g, 0)
            dkv_all = lax.dynamic_update_index_in_dim(dkv_all, dkv[:, :2], core * n_grp + g, 0)
            dkv_all = lax.dynamic_update_index_in_dim(dkv_all, swap(dkv[:, 2:], 1), (1 - core) * n_grp + g, 0)

        grad_query = dq_all.transpose(1, 3, 0, 2, 4).reshape(tok_dev, n_heads, head_dim)
        grad_kv = dkv_all.transpose(1, 2, 3, 0, 4).reshape(2, tok_dev, kv_heads, head_dim)
        return grad_query, grad_kv[0], grad_kv[1]

    return jax.shard_map(local_grads, mesh=mesh, in_specs=(row_spec, row_spec, row_spec, row_spec, row_spec, stat_spec), out_specs=(row_spec, row_spec, row_spec), check_vma=False)
```
